32 devices in a mesh: rep: 4 (over y, z), shard: 8 (over x, core).
Axes of the slice: x: 4, y: 2, z: 2, core: 2. Of those that a mesh axis runs over, the one named last changes fastest.
The devices are a block of a 4x4x8 slice.
Arguments:
- ratings: float32 [4096, 4096], P(('rep', 'shard')), parts along dimension 0
- observed: int32 [4096, 4096], P(('rep', 'shard')), parts along dimension 0
- user_init: float32 [4096, 32], P(('rep', 'shard')), parts along dimension 0
- item_init: float32 [16384, 32], P(('rep', 'shard')), parts along dimension 0
Outputs:
- output 1: float32 [4096, 32], P(('rep', 'shard')), parts along dimension 0
- output 2: float32 [16384, 32], P(('rep', 'shard')), parts along dimension 0
There are 4 independent parts. The reference program is written for one: setup_inputs(seed, part) draws one part's arguments, and reference() takes and returns one part's arrays. A program takes and returns all parts, laid end to end along the dimension named above; each array names one.
All inputs are finite; a program needn't handle non-finite values.
Results may differ from the reference program's by a relative error of at most 0.001.
Values are sent between devices in bfloat16 or wider.
A program may use at most 768 MiB of HBM per device.

```python
import jax
import jax.numpy as jnp
import math
from jax import lax

GROUP_DEVS = 8
USERS_DEV = 128
ITEMS_DEV = 512
FACTOR_RANK = 32
STRATUM_STEPS = 4
EPOCHS = 2

USERS = USERS_DEV * GROUP_DEVS
ITEMS = ITEMS_DEV * GROUP_DEVS
STEP_SCALE = (USERS_DEV + ITEMS_DEV + FACTOR_RANK) / math.sqrt(FACTOR_RANK)
STEP_SIZE = 0.5 / STEP_SCALE
WEIGHT_DECAY = 0.03 * math.sqrt(USERS_DEV * ITEMS_DEV / FACTOR_RANK)


def setup_inputs(seed: int = 0, part: int = 0) -> dict:
    base_key = jax.random.fold_in(jax.random.key(seed), part)
    sub_keys = jax.random.split(base_key, 6)
    init_scale = FACTOR_RANK ** -0.25
    true_users = jax.random.normal(sub_keys[0], (USERS, FACTOR_RANK), jnp.float32) * init_scale
    true_items = jax.random.normal(sub_keys[1], (ITEMS, FACTOR_RANK), jnp.float32) * init_scale
    rating_noise = 0.3 * jax.random.normal(sub_keys[2], (USERS, ITEMS), jnp.float32)
    ratings = jnp.dot(true_users, true_items.T) + rating_noise
    observed = (jax.random.randint(sub_keys[3], (USERS, ITEMS), 0, 10) < 3).astype(jnp.int32)
    user_init = jax.random.normal(sub_keys[4], (USERS, FACTOR_RANK), jnp.float32) * init_scale
    item_init = jax.random.normal(sub_keys[5], (ITEMS, FACTOR_RANK), jnp.float32) * init_scale
    return {"ratings": ratings, "observed": observed, "user_init": user_init, "item_init": item_init}


def to_bf16(values):
    return values.astype(jnp.bfloat16).astype(jnp.float32)


def reference(ratings, observed, user_init, item_init):
    rating_grid = ratings.reshape(GROUP_DEVS, USERS_DEV, GROUP_DEVS, ITEMS_DEV)
    seen_grid = (observed != 0).reshape(GROUP_DEVS, USERS_DEV, GROUP_DEVS, ITEMS_DEV)
    dev_ids = jnp.arange(GROUP_DEVS)
    user_blocks = user_init.reshape(GROUP_DEVS, USERS_DEV, FACTOR_RANK)
    held_items = item_init.reshape(GROUP_DEVS, ITEMS_DEV, FACTOR_RANK)

    def stratum(loop_state, stratum_idx):
        user_now, held_now = loop_state
        col_ids = (dev_ids + stratum_idx) % GROUP_DEVS
        rating_blk = rating_grid[dev_ids, :, col_ids]
        seen_blk = seen_grid[dev_ids, :, col_ids]

        def step(state_pair, unused):
            user_cur, item_cur = state_pair
            item_bf = to_bf16(item_cur)
            predicted = jnp.einsum("pur,pir->pui", to_bf16(user_cur), item_bf)
            residual = to_bf16(jnp.where(seen_blk, predicted - rating_blk, 0.0))
            user_new = user_cur - STEP_SIZE * (jnp.einsum("pui,pir->pur", residual, item_bf) + WEIGHT_DECAY * user_cur)
            user_bf = to_bf16(user_new)
            predicted = jnp.einsum("pur,pir->pui", user_bf, item_bf)
            residual = to_bf16(jnp.where(seen_blk, predicted - rating_blk, 0.0))
            item_new = item_cur - STEP_SIZE * (jnp.einsum("pui,pur->pir", residual, user_bf) + WEIGHT_DECAY * item_cur)
            return (user_new, item_new), None

        (user_now, held_now), unused = lax.scan(step, (user_now, held_now), None, length=STRATUM_STEPS)
        held_now = jnp.roll(held_now, -1, axis=0)
        return (user_now, held_now), None

    stratum_order = jnp.tile(dev_ids, EPOCHS)
    (user_blocks, held_items), unused = lax.scan(stratum, (user_blocks, held_items), stratum_order)
    return user_blocks.reshape(USERS, FACTOR_RANK), held_items.reshape(ITEMS, FACTOR_RANK)
```

```python
import functools
import math

import jax
import jax.numpy as jnp
from jax import lax
from jax.experimental import pallas as pl
from jax.experimental.pallas import tpu as pltpu
from jax.sharding import PartitionSpec as P

STRATUM_STEPS = 4
EPOCHS = 2
MESH = pl.DeviceIdType.MESH
BF16 = jnp.bfloat16
F32 = jnp.float32


def kernel(group, ratings, observed, user_t, item_t, user_out, item_out,
           rate, seen, held, sent, rate_sem, seen_sem, send_sem, recv_sem):
    me = lax.axis_index("shard")
    left, right = lax.rem(me + group - 1, group), lax.rem(me + 1, group)
    rank, users = user_t.shape
    items = item_t.shape[1]
    step_scale = (users + items + rank) / math.sqrt(rank)
    step_size = 0.5 / step_scale
    weight_decay = 0.03 * math.sqrt(users * items / rank)
    strata = EPOCHS * group

    def fetches(stratum):
        start = pl.multiple_of(lax.rem(me + stratum, group) * items, items)
        return (
            pltpu.make_async_copy(ratings.at[:, pl.ds(start, items)], rate.at[stratum], rate_sem.at[stratum]),
            pltpu.make_async_copy(observed.at[:, pl.ds(start, items)], seen.at[stratum], seen_sem.at[stratum]),
        )

    for stratum in range(group):
        for fetch in fetches(stratum):
            fetch.start()

    barrier = pltpu.get_barrier_semaphore()
    for neighbour in (left, right):
        pl.semaphore_signal(barrier, inc=1, device_id={"shard": neighbour}, device_id_type=MESH)
    pl.semaphore_wait(barrier, 2)

    held[0] = item_t[...]

    def hop(stratum):
        return pltpu.make_async_remote_copy(
            src_ref=sent.at[stratum],
            dst_ref=held.at[stratum + 1],
            send_sem=send_sem.at[stratum],
            recv_sem=recv_sem.at[stratum],
            device_id={"shard": left},
            device_id_type=MESH,
        )

    def half(user_bf, item_bf, seen_blk, rate_blk):
        predicted = jnp.dot(user_bf, item_bf, preferred_element_type=F32)
        return jnp.where(seen_blk, predicted - rate_blk, 0.0).astype(BF16)

    def stratum_body(stratum, user):
        block = lax.rem(stratum, group)

        @pl.when(stratum < group)
        def _():
            for fetch in fetches(block):
                fetch.wait()

        @pl.when(stratum > 0)
        def _():
            hop(stratum - 1).wait_recv()

        item = held[stratum]
        for _ in range(STRATUM_STEPS):
            item_bf = item.astype(BF16)
            residual = half(user.astype(BF16), item_bf, seen[block] != 0, rate[block])
            grad_user = lax.dot_general(residual, item_bf, (((1,), (1,)), ((), ())), preferred_element_type=F32)
            user = user - step_size * (grad_user + weight_decay * user)
            user_bf = user.astype(BF16)
            residual = half(user_bf, item_bf, seen[block] != 0, rate[block])
            grad_item = jnp.dot(user_bf.T, residual, preferred_element_type=F32)
            item = item - step_size * (grad_item + weight_decay * item)
        sent[stratum] = item
        hop(stratum).start()
        return user

    user = lax.fori_loop(0, strata, stratum_body, user_t[...].T)
    user_out[...] = user.T
    for stratum in range(strata):
        hop(stratum).wait_send()
    hop(strata - 1).wait_recv()
    item_out[...] = held[strata]


def solution(mesh):
    group = mesh.shape["shard"]
    row_spec = P(("rep", "shard"), None)
    strata = EPOCHS * group

    def local(ratings, observed, user_init, item_init):
        users, rank = user_init.shape
        items = item_init.shape[0]
        vmem = pl.BlockSpec(memory_space=pltpu.VMEM)
        hbm = pl.BlockSpec(memory_space=pl.ANY)
        user_t, item_t = pl.pallas_call(
            functools.partial(kernel, group),
            out_shape=(
                jax.ShapeDtypeStruct((rank, users), F32),
                jax.ShapeDtypeStruct((rank, items), F32),
            ),
            in_specs=[hbm, hbm, vmem, vmem],
            out_specs=(vmem, vmem),
            scratch_shapes=[
                pltpu.VMEM((group, users, items), F32),
                pltpu.VMEM((group, users, items), jnp.int32),
                pltpu.VMEM((strata + 1, rank, items), F32),
                pltpu.VMEM((strata, rank, items), F32),
                pltpu.SemaphoreType.DMA((group,)),
                pltpu.SemaphoreType.DMA((group,)),
                pltpu.SemaphoreType.DMA((strata,)),
                pltpu.SemaphoreType.DMA((strata,)),
            ],
            compiler_params=pltpu.CompilerParams(collective_id=0, has_side_effects=True),
        )(ratings, observed, user_init.T, item_init.T)
        return user_t.T, item_t.T

    return jax.shard_map(local, mesh=mesh, in_specs=(row_spec,) * 4, out_specs=(row_spec, row_spec), check_vma=False)
```
